128 devices in a mesh: rec: 4 (over z), space: 32 (over y, x, core).
Axes of the slice: x: 4, y: 4, z: 4, core: 2. Of those that a mesh axis runs over, the one named last changes fastest.
Arguments:
- probes: bfloat16 [1048576, 128], P('space'), may hold values from -6 to 6
- band_coeffs: bfloat16 [16, 8, 1048576], P('rec', None, 'space'), may hold values from -2 to 2
- band_offsets: int32 [16, 8], P('rec'), may hold values from -128 to 128, as said below
Outputs:
- q_basis: float32 [1048576, 128], P(('space', 'rec'))
- r_factor: float32 [128, 128], replicated
The draws below stay inside these ranges and needn't reach their ends.
Inputs may be any that keep to these rules, and one draw needn't show every extreme that they name: `band_offsets`: in every record band 0 has offset -128 and band 1 offset 128.
All inputs are finite; a program needn't handle non-finite values.
Results may differ from the reference program's by a relative error of at most 0.0003.
Values may be sent and summed in bfloat16 or wider, within the bound.
A program may use at most 128 MiB of HBM per device.

```python
import jax
import jax.numpy as jnp
from jax import lax

K = 128
NB = 8
HALO = 128
NREC = 16
PARAMS = 1048576


def draw_band_offsets(key, part):
    inner = jax.random.randint(jax.random.fold_in(key, 7), (NREC, NB - 2), -HALO, HALO + 1)
    left = jnp.full((NREC, 1), -HALO, jnp.int32)
    right = jnp.full((NREC, 1), HALO, jnp.int32)
    return jnp.concatenate([left, right, inner.astype(jnp.int32)], axis=1)


def levels(key, dims, pieces, low, largest):
    factor_of = 1.0
    for axis_at, blocks in pieces:
        steps = jax.random.uniform(jax.random.fold_in(jax.random.fold_in(key, 6), axis_at), (blocks,), jnp.float32, low / len(pieces), largest / len(pieces))
        factor_of = factor_of * jnp.repeat(jnp.exp(steps), dims[axis_at] // blocks).reshape((-1,) + (1,) * (len(dims) - 1 - axis_at))
    return factor_of


def scatter_about(key, extent, scale, bound, pieces=(), kind=jnp.bfloat16):
    gain = levels(key, extent, pieces, -0.22, 0.18) if pieces else 1.0
    array = jax.random.normal(key, extent, jnp.float32) * scale * gain
    return jnp.minimum(jnp.maximum(array, -bound), bound).astype(kind)


def setup_inputs(seed: int = 0) -> dict:
    key_of = jax.random.split(jax.random.key(seed), 4)
    return {
        "probes": scatter_about(key_of[0], (PARAMS, K), 1.0, 6.0, ((0, 32),)),
        "band_coeffs": scatter_about(key_of[1], (NREC, NB, PARAMS), 0.25, 2.0, ((0, 4), (2, 32))),
        "band_offsets": draw_band_offsets(jax.random.fold_in(key_of[3], 71), 0),
    }


def reference(probes, band_coeffs, band_offsets):
    padded = jnp.pad(probes.astype(jnp.float32), ((HALO, HALO), (0, 0)))

    def step(index, acc):
        record = index // NB
        band = index % NB
        offset = band_offsets[record, band]
        rows = lax.dynamic_slice_in_dim(padded, (HALO + offset).astype(jnp.int32), PARAMS, 0)
        return acc + band_coeffs[record, band].astype(jnp.float32)[:, None] * rows
    sketch = lax.fori_loop(0, NREC * NB, step, jnp.zeros((PARAMS, K), jnp.float32))
    gram = jnp.dot(sketch.T.astype(jnp.float32), sketch.astype(jnp.float32), precision=lax.Precision.HIGHEST, preferred_element_type=jnp.float32)
    lower = jnp.linalg.cholesky(gram)
    scale = jnp.sqrt(jnp.float32(PARAMS))
    solved = jax.scipy.linalg.solve_triangular(lower, sketch.T, lower=True)
    return (solved.T * scale, lower.T / scale)
```

```python
import functools
import math

import jax
import jax.numpy as jnp
from jax import lax
from jax.experimental import pallas as pl
from jax.experimental.pallas import tpu as pltpu
from jax.sharding import PartitionSpec as P

HALO = 128
B = 128
CHUNK = 1024
UNROLL = 4
MESH = pl.DeviceIdType.MESH
F32 = jnp.float32
BF16 = jnp.bfloat16


def dot(a, b, dims):
    return lax.dot_general(a, b, (dims, ((), ())), preferred_element_type=F32)


def split(x):
    high = x.astype(BF16)
    low = (x - high.astype(F32)).astype(BF16)
    return high, low


def sketch_kernel(
    nr, ns, c_hbm, o_hbm, p_hbm, hl_ref, g_ref,
    cbuf, obuf, sel, pbuf, c_send, c_recv, o_send, o_recv, h_send, h_recv, local_sem, own_sem,
):
    r = lax.axis_index("rec")
    s = lax.axis_index("space")
    share = cbuf.shape[1]
    nloc = c_hbm.shape[0]
    rows = p_hbm.shape[0]
    nch = share // CHUNK
    first, last = r == 0, r == nr - 1
    has_left, has_right = s > 0, s < ns - 1
    edge = jnp.logical_or(first, last)

    main = pltpu.make_async_copy(
        p_hbm.at[pl.ds(pl.multiple_of(r * share, share), share)],
        pbuf.at[pl.ds(HALO, share)], local_sem.at[0])
    main.start()

    def own_c(ch):
        return pltpu.make_async_copy(
            c_hbm.at[:, pl.ds(pl.multiple_of(r * share + ch * CHUNK, CHUNK), CHUNK)],
            cbuf.at[pl.ds(pl.multiple_of(r * nloc, nloc), nloc), pl.ds(pl.multiple_of(ch * CHUNK, CHUNK), CHUNK)],
            own_sem.at[ch])

    for ch in range(nch):
        own_c(ch).start()
    own_o = pltpu.make_async_copy(
        o_hbm, obuf.at[pl.ds(pl.multiple_of(r * nloc, nloc), nloc)], local_sem.at[1])
    own_o.start()

    barrier = pltpu.get_barrier_semaphore()
    for k in range(1, nr):
        pl.semaphore_signal(barrier, inc=1, device_id={"rec": lax.rem(r + k, nr)}, device_id_type=MESH)

    @pl.when(jnp.logical_and(edge, has_left))
    def _():
        pl.semaphore_signal(barrier, inc=1, device_id={"space": s - 1}, device_id_type=MESH)

    @pl.when(jnp.logical_and(edge, has_right))
    def _():
        pl.semaphore_signal(barrier, inc=1, device_id={"space": s + 1}, device_id_type=MESH)

    on_edge = edge.astype(jnp.int32)
    peers = nr - 1 + on_edge * (has_left.astype(jnp.int32) + has_right.astype(jnp.int32))
    pl.semaphore_wait(barrier, peers)

    def send_o(k):
        return pltpu.make_async_remote_copy(
            src_ref=o_hbm, dst_ref=obuf.at[pl.ds(pl.multiple_of(r * nloc, nloc), nloc)],
            send_sem=o_send.at[k - 1], recv_sem=o_recv.at[k - 1],
            device_id={"rec": lax.rem(r + k, nr)}, device_id_type=MESH)

    def recv_o(k):
        src = lax.rem(r + nr - k, nr)
        return pltpu.make_async_remote_copy(
            src_ref=o_hbm, dst_ref=obuf.at[pl.ds(pl.multiple_of(src * nloc, nloc), nloc)],
            send_sem=o_send.at[k - 1], recv_sem=o_recv.at[k - 1],
            device_id={"rec": lax.rem(r + k, nr)}, device_id_type=MESH)

    def send_c(k, ch):
        to = lax.rem(r + k, nr)
        return pltpu.make_async_remote_copy(
            src_ref=c_hbm.at[:, pl.ds(pl.multiple_of(to * share + ch * CHUNK, CHUNK), CHUNK)],
            dst_ref=cbuf.at[pl.ds(pl.multiple_of(r * nloc, nloc), nloc), pl.ds(pl.multiple_of(ch * CHUNK, CHUNK), CHUNK)],
            send_sem=c_send.at[k - 1, ch], recv_sem=c_recv.at[k - 1, ch],
            device_id={"rec": to}, device_id_type=MESH)

    def recv_c(k, ch):
        src = lax.rem(r + nr - k, nr)
        return pltpu.make_async_remote_copy(
            src_ref=c_hbm.at[:, pl.ds(0, CHUNK)],
            dst_ref=cbuf.at[pl.ds(pl.multiple_of(src * nloc, nloc), nloc), pl.ds(pl.multiple_of(ch * CHUNK, CHUNK), CHUNK)],
            send_sem=c_send.at[k - 1, ch], recv_sem=c_recv.at[k - 1, ch],
            device_id={"rec": lax.rem(r + k, nr)}, device_id_type=MESH)

    for k in range(1, nr):
        send_o(k).start()

    tail = pltpu.make_async_remote_copy(
        src_ref=p_hbm.at[pl.ds(rows - HALO, HALO)], dst_ref=pbuf.at[pl.ds(0, HALO)],
        send_sem=h_send.at[0], recv_sem=h_recv.at[0],
        device_id={"space": lax.rem(s + 1, ns)}, device_id_type=MESH)
    head = pltpu.make_async_remote_copy(
        src_ref=p_hbm.at[pl.ds(0, HALO)], dst_ref=pbuf.at[pl.ds(share + HALO, HALO)],
        send_sem=h_send.at[1], recv_sem=h_recv.at[1],
        device_id={"space": lax.rem(s + ns - 1, ns)}, device_id_type=MESH)

    @pl.when(jnp.logical_and(first, has_right))
    def _():
        tail.start()

    @pl.when(jnp.logical_and(last, has_left))
    def _():
        head.start()

    for ch in range(nch):
        for k in (2, 1, 3):
            send_c(k, ch).start()

    @pl.when(jnp.logical_and(first, s == 0))
    def _():
        pbuf[pl.ds(0, HALO), :] = jnp.zeros((HALO, pbuf.shape[1]), BF16)

    @pl.when(jnp.logical_and(last, s == ns - 1))
    def _():
        pbuf[pl.ds(share + HALO, HALO), :] = jnp.zeros((HALO, pbuf.shape[1]), BF16)

    @pl.when(r > 0)
    def _():
        cp = pltpu.make_async_copy(
            p_hbm.at[pl.ds(pl.multiple_of(r * share - HALO, HALO), HALO)],
            pbuf.at[pl.ds(0, HALO)], local_sem.at[2])
        cp.start()
        cp.wait()

    @pl.when(r < nr - 1)
    def _():
        cp = pltpu.make_async_copy(
            p_hbm.at[pl.ds(pl.multiple_of((r + 1) * share, HALO), HALO)],
            pbuf.at[pl.ds(share + HALO, HALO)], local_sem.at[3])
        cp.start()
        cp.wait()

    @pl.when(jnp.logical_and(first, has_left))
    def _():
        tail.wait_recv()

    @pl.when(jnp.logical_and(last, has_right))
    def _():
        head.wait_recv()

    own_o.wait()
    for k in range(1, nr):
        recv_o(k).wait_recv()
    off = obuf[...]
    lane = lax.broadcasted_iota(jnp.int32, (B, B), 1)
    for t in range(3):
        sel[:, t * B:(t + 1) * B] = jnp.where(lane + (t * B - HALO) == off, 1.0, 0.0).astype(BF16)
    main.wait()
    g_ref[...] = jnp.zeros_like(g_ref)

    def block(p0):
        cols = cbuf[:, pl.ds(p0, B)]
        diag = dot(cols, sel[...], ((0,), (0,)))
        band = pltpu.roll(diag, 0, 1, stride=1, stride_axis=0)
        bh, bl = split(band)
        piece = pbuf[pl.ds(p0, 3 * B), :]
        sk = dot(bh, piece, ((1,), (0,))) + dot(bl, piece, ((1,), (0,)))
        hi, lo = split(sk)
        hl_ref[pl.ds(p0, B), 0:B] = hi
        hl_ref[pl.ds(p0, B), B:2 * B] = lo

    def step(i, _):
        base = pl.multiple_of(i * (UNROLL * B), UNROLL * B)
        for u in range(UNROLL):
            block(base + u * B)
        hl = hl_ref[pl.ds(base, UNROLL * B), :]
        g_ref[...] += dot(hl, hl, ((0,), (0,)))
        return 0

    def chunk(ch, _):
        own_c(ch).wait()
        for k in (1, 3, 2):
            recv_c(k, ch).wait_recv()
        per = CHUNK // (UNROLL * B)
        lax.fori_loop(ch * per, (ch + 1) * per, step, 0)
        return 0

    lax.fori_loop(0, nch, chunk, 0)

    for k in range(1, nr):
        send_o(k).wait_send()
        for ch in range(nch):
            send_c(k, ch).wait_send()

    @pl.when(jnp.logical_and(first, has_right))
    def _():
        tail.wait_send()

    @pl.when(jnp.logical_and(last, has_left))
    def _():
        head.wait_send()


def factor_kernel(scale, hl_ref, g_ref, q_ref, u_ref, w_ref):
    n = g_ref.shape[0]

    @pl.when(pl.program_id(0) == 0)
    def _():
        a = g_ref[...]
        rowi = lax.broadcasted_iota(jnp.int32, (n, n), 0)
        lane = lax.broadcasted_iota(jnp.int32, (n, n), 1)
        eye = jnp.where(rowi == lane, 1.0, 0.0).astype(F32)
        nt = n // 8
        at = [a[8 * t:8 * t + 8] for t in range(nt)]
        it = [eye[8 * t:8 * t + 8] for t in range(nt)]
        sub = lax.broadcasted_iota(jnp.int32, (8, n), 0)
        for j in range(n):
            t0 = j // 8
            ra = jnp.broadcast_to(at[t0][j % 8:j % 8 + 1, :], (8, n))
            ri = jnp.broadcast_to(it[t0][j % 8:j % 8 + 1, :], (8, n))
            piv = jnp.broadcast_to(ra[:, j:j + 1], (8, n))
            inv = 1.0 / piv
            ra = ra * inv
            ri = ri * inv
            for t in range(t0, nt):
                if t == t0 and j % 8 == 7:
                    continue
                col = jnp.broadcast_to(at[t][:, j:j + 1], (8, n))
                if t == t0:
                    col = jnp.where(sub > j % 8, col, 0.0)
                at[t] = at[t] - col * ra
                it[t] = it[t] - col * ri
        a = jnp.concatenate(at, axis=0)
        linv = jnp.concatenate(it, axis=0)
        diag = jnp.sum(jnp.where(rowi == lane, a, 0.0), axis=1, keepdims=True)
        rs = 1.0 / jnp.sqrt(diag)
        u_ref[...] = jnp.where(lane >= rowi, a, 0.0) * (rs * (1.0 / scale))
        linv = jnp.where(lane <= rowi, linv, 0.0) * (rs * scale)
        right = linv.T
        rh, rl = split(right)
        w_ref[0:n, 0:n] = rh
        w_ref[0:n, n:2 * n] = rl
        w_ref[n:2 * n, 0:n] = rh
        w_ref[n:2 * n, n:2 * n] = jnp.zeros((n, n), BF16)

    out = dot(hl_ref[...], w_ref[...], ((1,), (0,)))
    q_ref[...] = out[:, :n] + out[:, n:]


def local(nr, ns, probes, band_coeffs, band_offsets):
    rows, k = probes.shape
    share = rows // nr
    nloc = band_coeffs.shape[0] * band_coeffs.shape[1]
    nall = nr * nloc
    nch = share // CHUNK
    coeffs = band_coeffs.reshape(nloc, rows)
    offs = jnp.broadcast_to(band_offsets.reshape(nloc, 1), (nloc, B))
    any_spec = pl.BlockSpec(memory_space=pl.ANY)
    vmem_spec = pl.BlockSpec(memory_space=pltpu.VMEM)
    dma = pltpu.SemaphoreType.DMA
    hl, g = pl.pallas_call(
        functools.partial(sketch_kernel, nr, ns),
        out_shape=(jax.ShapeDtypeStruct((share, 2 * k), BF16), jax.ShapeDtypeStruct((2 * k, 2 * k), F32)),
        in_specs=[any_spec] * 3,
        out_specs=(vmem_spec, vmem_spec),
        scratch_shapes=[
            pltpu.VMEM((nall, share), BF16),
            pltpu.VMEM((nall, B), jnp.int32),
            pltpu.VMEM((nall, 3 * B), BF16),
            pltpu.VMEM((share + 2 * HALO, k), BF16),
            dma((nr - 1, nch)), dma((nr - 1, nch)),
            dma((nr - 1,)), dma((nr - 1,)), dma((2,)), dma((2,)), dma((4,)), dma((nch,)),
        ],
        compiler_params=pltpu.CompilerParams(
            collective_id=0, has_side_effects=True, vmem_limit_bytes=48 << 20),
    )(coeffs, offs, probes)
    gram = g[:k, :k] + g[:k, k:] + g[k:, :k] + g[k:, k:]
    gram = lax.psum(gram, ("rec", "space"))
    scale = math.sqrt(rows * ns)
    tile = 1024
    q, u = pl.pallas_call(
        functools.partial(factor_kernel, scale),
        grid=(share // tile,),
        out_shape=(jax.ShapeDtypeStruct((share, k), F32), jax.ShapeDtypeStruct((k, k), F32)),
        in_specs=[pl.BlockSpec((tile, 2 * k), lambda i: (i, 0)), pl.BlockSpec((k, k), lambda i: (0, 0))],
        out_specs=(pl.BlockSpec((tile, k), lambda i: (i, 0)), pl.BlockSpec((k, k), lambda i: (0, 0))),
        scratch_shapes=[pltpu.VMEM((2 * k, 2 * k), BF16)],
        compiler_params=pltpu.CompilerParams(dimension_semantics=("arbitrary",)),
    )(hl, gram)
    return q, u


def solution(mesh):
    in_specs = (P("space", None), P("rec", None, "space"), P("rec", None))
    out_specs = (P(("space", "rec"), None), P())
    body = functools.partial(local, mesh.shape["rec"], mesh.shape["space"])
    return jax.shard_map(body, mesh=mesh, in_specs=in_specs, out_specs=out_specs, check_vma=False)
```

```python
import functools
import math

import jax
import jax.numpy as jnp
from jax import lax
from jax.experimental import pallas as pl
from jax.experimental.pallas import tpu as pltpu
from jax.sharding import PartitionSpec as P

HALO = 128
SIDE = 4
B = 128
CHUNK = 1024
UNROLL = 4
MESH = pl.DeviceIdType.MESH
F32 = jnp.float32
BF16 = jnp.bfloat16


def dot(a, b, dims):
    return lax.dot_general(a, b, (dims, ((), ())), preferred_element_type=F32)


def split(x):
    high = x.astype(BF16)
    low = (x - high.astype(F32)).astype(BF16)
    return high, low


def sketch_kernel(
    nr, ns, c_hbm, o_hbm, p_hbm, hl_ref, out_ref,
    cbuf, obuf, sel, pbuf, g_ref, gsum, gpart, gx, gy, gall,
    c_send, c_recv, o_send, o_recv, h_send, h_recv, local_sem, own_sem,
    s_send, s_recv, x_send, x_recv, y_send, y_recv, a_send, a_recv,
):
    r = lax.axis_index("rec")
    s = lax.axis_index("space")
    share = cbuf.shape[1]
    nloc = c_hbm.shape[0]
    rows = p_hbm.shape[0]
    nch = share // CHUNK
    first, last = r == 0, r == nr - 1
    has_left, has_right = s > 0, s < ns - 1
    edge = jnp.logical_or(first, last)

    main = pltpu.make_async_copy(
        p_hbm.at[pl.ds(pl.multiple_of(r * share, share), share)],
        pbuf.at[pl.ds(HALO, share)], local_sem.at[0])
    main.start()

    def own_c(ch):
        return pltpu.make_async_copy(
            c_hbm.at[:, pl.ds(pl.multiple_of(r * share + ch * CHUNK, CHUNK), CHUNK)],
            cbuf.at[pl.ds(pl.multiple_of(r * nloc, nloc), nloc), pl.ds(pl.multiple_of(ch * CHUNK, CHUNK), CHUNK)],
            own_sem.at[ch])

    for ch in range(nch):
        own_c(ch).start()
    own_o = pltpu.make_async_copy(
        o_hbm, obuf.at[pl.ds(pl.multiple_of(r * nloc, nloc), nloc)], local_sem.at[1])
    own_o.start()

    core = lax.rem(s, 2)
    xi = lax.rem(s // 2, SIDE)
    yi = s // (2 * SIDE)
    octet = 2 * nr
    mine = 2 * r + core

    def cube_peer(k):
        at = lax.rem(mine + k, octet)
        return at, {"rec": at // 2, "space": s - core + lax.rem(at, 2)}

    def x_peer(k):
        return {"space": s + 2 * (lax.rem(xi + k, SIDE) - xi)}

    def y_peer(k):
        return {"space": s + 2 * SIDE * (lax.rem(yi + k, SIDE) - yi)}

    barrier = pltpu.get_barrier_semaphore()
    for k in range(1, octet):
        pl.semaphore_signal(barrier, inc=1, device_id=cube_peer(k)[1], device_id_type=MESH)
    for k in range(1, SIDE):
        pl.semaphore_signal(barrier, inc=1, device_id=x_peer(k), device_id_type=MESH)
        pl.semaphore_signal(barrier, inc=1, device_id=y_peer(k), device_id_type=MESH)

    other = s + 2 * core - 1
    has_other = jnp.logical_and(edge, jnp.logical_and(other >= 0, other < ns))

    @pl.when(has_other)
    def _():
        pl.semaphore_signal(barrier, inc=1, device_id={"space": other}, device_id_type=MESH)

    pl.semaphore_wait(barrier, octet - 1 + 2 * (SIDE - 1) + has_other.astype(jnp.int32))

    def send_o(k):
        return pltpu.make_async_remote_copy(
            src_ref=o_hbm, dst_ref=obuf.at[pl.ds(pl.multiple_of(r * nloc, nloc), nloc)],
            send_sem=o_send.at[k - 1], recv_sem=o_recv.at[k - 1],
            device_id={"rec": lax.rem(r + k, nr)}, device_id_type=MESH)

    def recv_o(k):
        src = lax.rem(r + nr - k, nr)
        return pltpu.make_async_remote_copy(
            src_ref=o_hbm, dst_ref=obuf.at[pl.ds(pl.multiple_of(src * nloc, nloc), nloc)],
            send_sem=o_send.at[k - 1], recv_sem=o_recv.at[k - 1],
            device_id={"rec": lax.rem(r + k, nr)}, device_id_type=MESH)

    def send_c(k, ch):
        to = lax.rem(r + k, nr)
        return pltpu.make_async_remote_copy(
            src_ref=c_hbm.at[:, pl.ds(pl.multiple_of(to * share + ch * CHUNK, CHUNK), CHUNK)],
            dst_ref=cbuf.at[pl.ds(pl.multiple_of(r * nloc, nloc), nloc), pl.ds(pl.multiple_of(ch * CHUNK, CHUNK), CHUNK)],
            send_sem=c_send.at[k - 1, ch], recv_sem=c_recv.at[k - 1, ch],
            device_id={"rec": to}, device_id_type=MESH)

    def recv_c(k, ch):
        src = lax.rem(r + nr - k, nr)
        return pltpu.make_async_remote_copy(
            src_ref=c_hbm.at[:, pl.ds(0, CHUNK)],
            dst_ref=cbuf.at[pl.ds(pl.multiple_of(src * nloc, nloc), nloc), pl.ds(pl.multiple_of(ch * CHUNK, CHUNK), CHUNK)],
            send_sem=c_send.at[k - 1, ch], recv_sem=c_recv.at[k - 1, ch],
            device_id={"rec": lax.rem(r + k, nr)}, device_id_type=MESH)

    for k in range(1, nr):
        send_o(k).start()

    tail = pltpu.make_async_remote_copy(
        src_ref=p_hbm.at[pl.ds(rows - HALO, HALO)], dst_ref=pbuf.at[pl.ds(0, HALO)],
        send_sem=h_send.at[0], recv_sem=h_recv.at[0],
        device_id={"space": lax.rem(s + 1, ns)}, device_id_type=MESH)
    head = pltpu.make_async_remote_copy(
        src_ref=p_hbm.at[pl.ds(0, HALO)], dst_ref=pbuf.at[pl.ds(share + HALO, HALO)],
        send_sem=h_send.at[1], recv_sem=h_recv.at[1],
        device_id={"space": lax.rem(s + ns - 1, ns)}, device_id_type=MESH)

    @pl.when(jnp.logical_and(first, has_right))
    def _():
        tail.start()

    @pl.when(jnp.logical_and(last, has_left))
    def _():
        head.start()

    for ch in range(nch):
        for k in (2, 1, 3):
            send_c(k, ch).start()

    @pl.when(jnp.logical_and(first, s == 0))
    def _():
        pbuf[pl.ds(0, HALO), :] = jnp.zeros((HALO, pbuf.shape[1]), BF16)

    @pl.when(jnp.logical_and(last, s == ns - 1))
    def _():
        pbuf[pl.ds(share + HALO, HALO), :] = jnp.zeros((HALO, pbuf.shape[1]), BF16)

    @pl.when(r > 0)
    def _():
        cp = pltpu.make_async_copy(
            p_hbm.at[pl.ds(pl.multiple_of(r * share - HALO, HALO), HALO)],
            pbuf.at[pl.ds(0, HALO)], local_sem.at[2])
        cp.start()
        cp.wait()

    @pl.when(r < nr - 1)
    def _():
        cp = pltpu.make_async_copy(
            p_hbm.at[pl.ds(pl.multiple_of((r + 1) * share, HALO), HALO)],
            pbuf.at[pl.ds(share + HALO, HALO)], local_sem.at[3])
        cp.start()
        cp.wait()

    @pl.when(jnp.logical_and(first, has_left))
    def _():
        tail.wait_recv()

    @pl.when(jnp.logical_and(last, has_right))
    def _():
        head.wait_recv()

    own_o.wait()
    for k in range(1, nr):
        recv_o(k).wait_recv()
    off = obuf[...]
    lane = lax.broadcasted_iota(jnp.int32, (B, B), 1)
    for t in range(3):
        sel[:, t * B:(t + 1) * B] = jnp.where(lane + (t * B - HALO) == off, 1.0, 0.0).astype(BF16)
    main.wait()
    g_ref[...] = jnp.zeros_like(g_ref)

    def block(p0):
        cols = cbuf[:, pl.ds(p0, B)]
        diag = dot(cols, sel[...], ((0,), (0,)))
        band = pltpu.roll(diag, 0, 1, stride=1, stride_axis=0)
        bh, bl = split(band)
        piece = pbuf[pl.ds(p0, 3 * B), :]
        sk = dot(bh, piece, ((1,), (0,))) + dot(bl, piece, ((1,), (0,)))
        hi, lo = split(sk)
        hl_ref[pl.ds(p0, B), 0:B] = hi
        hl_ref[pl.ds(p0, B), B:2 * B] = lo

    def step(i, _):
        base = pl.multiple_of(i * (UNROLL * B), UNROLL * B)
        for u in range(UNROLL):
            block(base + u * B)
        hl = hl_ref[pl.ds(base, UNROLL * B), :]
        g_ref[...] += dot(hl, hl, ((0,), (0,)))
        return 0

    def chunk(ch, _):
        own_c(ch).wait()
        for k in (1, 3, 2):
            recv_c(k, ch).wait_recv()
        per = CHUNK // (UNROLL * B)
        lax.fori_loop(ch * per, (ch + 1) * per, step, 0)
        return 0

    lax.fori_loop(0, nch, chunk, 0)

    n = out_ref.shape[0]
    part = n // octet
    gsum[...] = (g_ref[0:n, 0:n] + g_ref[n:2 * n, n:2 * n]) + (g_ref[0:n, n:2 * n] + g_ref[n:2 * n, 0:n])

    def exchange(copies):
        for cp in copies:
            cp.start()
        for cp in copies:
            cp.wait_recv()

    def total(ref):
        acc = ref[0]
        for i in range(1, ref.shape[0]):
            acc = acc + ref[i]
        return acc

    scatter = []
    for k in range(1, octet):
        at, to = cube_peer(k)
        scatter.append(pltpu.make_async_remote_copy(
            src_ref=gsum.at[pl.ds(pl.multiple_of(at * part, part), part)], dst_ref=gpart.at[mine],
            send_sem=s_send.at[k - 1], recv_sem=s_recv.at[k - 1], device_id=to, device_id_type=MESH))
    gpart[mine] = gsum[pl.ds(pl.multiple_of(mine * part, part), part), :]
    exchange(scatter)
    gx[xi] = total(gpart)
    along_x = [pltpu.make_async_remote_copy(
        src_ref=gx.at[xi], dst_ref=gx.at[xi], send_sem=x_send.at[k - 1], recv_sem=x_recv.at[k - 1],
        device_id=x_peer(k), device_id_type=MESH) for k in range(1, SIDE)]
    exchange(along_x)
    gy[yi] = total(gx)
    along_y = [pltpu.make_async_remote_copy(
        src_ref=gy.at[yi], dst_ref=gy.at[yi], send_sem=y_send.at[k - 1], recv_sem=y_recv.at[k - 1],
        device_id=y_peer(k), device_id_type=MESH) for k in range(1, SIDE)]
    exchange(along_y)
    own = pl.ds(pl.multiple_of(mine * part, part), part)
    gall[own, :] = total(gy)
    gather = [pltpu.make_async_remote_copy(
        src_ref=gall.at[own], dst_ref=gall.at[own], send_sem=a_send.at[k - 1], recv_sem=a_recv.at[k - 1],
        device_id=cube_peer(k)[1], device_id_type=MESH) for k in range(1, octet)]
    exchange(gather)
    out_ref[...] = gall[...]
    for cp in scatter + along_x + along_y + gather:
        cp.wait_send()

    for k in range(1, nr):
        send_o(k).wait_send()
        for ch in range(nch):
            send_c(k, ch).wait_send()

    @pl.when(jnp.logical_and(first, has_right))
    def _():
        tail.wait_send()

    @pl.when(jnp.logical_and(last, has_left))
    def _():
        head.wait_send()


def factor_kernel(scale, hl_ref, g_ref, q_ref, u_ref, w_ref):
    n = g_ref.shape[0]

    @pl.when(pl.program_id(0) == 0)
    def _():
        a = g_ref[...]
        rowi = lax.broadcasted_iota(jnp.int32, (n, n), 0)
        lane = lax.broadcasted_iota(jnp.int32, (n, n), 1)
        eye = jnp.where(rowi == lane, 1.0, 0.0).astype(F32)
        nt = n // 8
        at = [a[8 * t:8 * t + 8] for t in range(nt)]
        it = [eye[8 * t:8 * t + 8] for t in range(nt)]
        sub = lax.broadcasted_iota(jnp.int32, (8, n), 0)
        for j in range(n):
            t0 = j // 8
            ra = jnp.broadcast_to(at[t0][j % 8:j % 8 + 1, :], (8, n))
            ri = jnp.broadcast_to(it[t0][j % 8:j % 8 + 1, :], (8, n))
            piv = jnp.broadcast_to(ra[:, j:j + 1], (8, n))
            inv = 1.0 / piv
            ra = ra * inv
            ri = ri * inv
            for t in range(t0, nt):
                if t == t0 and j % 8 == 7:
                    continue
                col = jnp.broadcast_to(at[t][:, j:j + 1], (8, n))
                if t == t0:
                    col = jnp.where(sub > j % 8, col, 0.0)
                at[t] = at[t] - col * ra
                it[t] = it[t] - col * ri
        a = jnp.concatenate(at, axis=0)
        linv = jnp.concatenate(it, axis=0)
        diag = jnp.sum(jnp.where(rowi == lane, a, 0.0), axis=1, keepdims=True)
        rs = 1.0 / jnp.sqrt(diag)
        u_ref[...] = jnp.where(lane >= rowi, a, 0.0) * (rs * (1.0 / scale))
        linv = jnp.where(lane <= rowi, linv, 0.0) * (rs * scale)
        right = linv.T
        rh, rl = split(right)
        w_ref[0:n, 0:n] = rh
        w_ref[0:n, n:2 * n] = rl
        w_ref[n:2 * n, 0:n] = rh
        w_ref[n:2 * n, n:2 * n] = jnp.zeros((n, n), BF16)

    out = dot(hl_ref[...], w_ref[...], ((1,), (0,)))
    q_ref[...] = out[:, :n] + out[:, n:]


def local(nr, ns, probes, band_coeffs, band_offsets):
    rows, k = probes.shape
    share = rows // nr
    nloc = band_coeffs.shape[0] * band_coeffs.shape[1]
    nall = nr * nloc
    nch = share // CHUNK
    octet = 2 * nr
    coeffs = band_coeffs.reshape(nloc, rows)
    offs = jnp.broadcast_to(band_offsets.reshape(nloc, 1), (nloc, B))
    any_spec = pl.BlockSpec(memory_space=pl.ANY)
    vmem_spec = pl.BlockSpec(memory_space=pltpu.VMEM)
    dma = pltpu.SemaphoreType.DMA
    hl, gram = pl.pallas_call(
        functools.partial(sketch_kernel, nr, ns),
        out_shape=(jax.ShapeDtypeStruct((share, 2 * k), BF16), jax.ShapeDtypeStruct((k, k), F32)),
        in_specs=[any_spec] * 3,
        out_specs=(vmem_spec, vmem_spec),
        scratch_shapes=[
            pltpu.VMEM((nall, share), BF16),
            pltpu.VMEM((nall, B), jnp.int32),
            pltpu.VMEM((nall, 3 * B), BF16),
            pltpu.VMEM((share + 2 * HALO, k), BF16),
            pltpu.VMEM((2 * k, 2 * k), F32),
            pltpu.VMEM((k, k), F32),
            pltpu.VMEM((octet, k // octet, k), F32),
            pltpu.VMEM((SIDE, k // octet, k), F32),
            pltpu.VMEM((SIDE, k // octet, k), F32),
            pltpu.VMEM((k, k), F32),
            dma((nr - 1, nch)), dma((nr - 1, nch)),
            dma((nr - 1,)), dma((nr - 1,)), dma((2,)), dma((2,)), dma((4,)), dma((nch,)),
            dma((octet - 1,)), dma((octet - 1,)), dma((SIDE - 1,)), dma((SIDE - 1,)),
            dma((SIDE - 1,)), dma((SIDE - 1,)), dma((octet - 1,)), dma((octet - 1,)),
        ],
        compiler_params=pltpu.CompilerParams(
            collective_id=0, has_side_effects=True, vmem_limit_bytes=48 << 20),
    )(coeffs, offs, probes)
    scale = math.sqrt(rows * ns)
    tile = 1024
    q, u = pl.pallas_call(
        functools.partial(factor_kernel, scale),
        grid=(share // tile,),
        out_shape=(jax.ShapeDtypeStruct((share, k), F32), jax.ShapeDtypeStruct((k, k), F32)),
        in_specs=[pl.BlockSpec((tile, 2 * k), lambda i: (i, 0)), pl.BlockSpec((k, k), lambda i: (0, 0))],
        out_specs=(pl.BlockSpec((tile, k), lambda i: (i, 0)), pl.BlockSpec((k, k), lambda i: (0, 0))),
        scratch_shapes=[pltpu.VMEM((2 * k, 2 * k), BF16)],
        compiler_params=pltpu.CompilerParams(dimension_semantics=("arbitrary",)),
    )(hl, gram)
    return q, u


def solution(mesh):
    in_specs = (P("space", None), P("rec", None, "space"), P("rec", None))
    out_specs = (P(("space", "rec"), None), P())
    body = functools.partial(local, mesh.shape["rec"], mesh.shape["space"])
    return jax.shard_map(body, mesh=mesh, in_specs=in_specs, out_specs=out_specs, check_vma=False)
```

```python
import functools
import math

import jax
import jax.numpy as jnp
from jax import lax
from jax.experimental import pallas as pl
from jax.experimental.pallas import tpu as pltpu
from jax.sharding import PartitionSpec as P

HALO = 128
SIDE = 4
B = 128
CHUNK = 1024
UNROLL = 4
MESH = pl.DeviceIdType.MESH
F32 = jnp.float32
BF16 = jnp.bfloat16


def dot(a, b, dims):
    return lax.dot_general(a, b, (dims, ((), ())), preferred_element_type=F32)


def split(x):
    high = x.astype(BF16)
    low = (x - high.astype(F32)).astype(BF16)
    return high, low


def sketch_kernel(
    nr, ns, c_hbm, o_hbm, p_hbm, hl_hbm, out_ref,
    hl_ref, cbuf, obuf, sel, pbuf, g_ref, gsum, gpart, gx, gy, gall,
    c_send, c_recv, o_send, o_recv, h_send, h_recv, local_sem, own_sem, out_sem,
    s_send, s_recv, x_send, x_recv, y_send, y_recv, a_send, a_recv,
):
    r = lax.axis_index("rec")
    s = lax.axis_index("space")
    share = cbuf.shape[1]
    nloc = c_hbm.shape[0]
    rows = p_hbm.shape[0]
    nch = share // CHUNK
    first, last = r == 0, r == nr - 1
    has_left, has_right = s > 0, s < ns - 1
    edge = jnp.logical_or(first, last)

    main = pltpu.make_async_copy(
        p_hbm.at[pl.ds(pl.multiple_of(r * share, share), share)],
        pbuf.at[pl.ds(HALO, share)], local_sem.at[0])
    main.start()

    def own_c(ch):
        return pltpu.make_async_copy(
            c_hbm.at[:, pl.ds(pl.multiple_of(r * share + ch * CHUNK, CHUNK), CHUNK)],
            cbuf.at[pl.ds(pl.multiple_of(r * nloc, nloc), nloc), pl.ds(pl.multiple_of(ch * CHUNK, CHUNK), CHUNK)],
            own_sem.at[ch])

    for ch in range(nch):
        own_c(ch).start()
    own_o = pltpu.make_async_copy(
        o_hbm, obuf.at[pl.ds(pl.multiple_of(r * nloc, nloc), nloc)], local_sem.at[1])
    own_o.start()

    core = lax.rem(s, 2)
    xi = lax.rem(s // 2, SIDE)
    yi = s // (2 * SIDE)
    octet = 2 * nr
    mine = 2 * r + core

    def cube_peer(k):
        at = lax.rem(mine + k, octet)
        return at, {"rec": at // 2, "space": s - core + lax.rem(at, 2)}

    def x_peer(k):
        return {"space": s + 2 * (lax.rem(xi + k, SIDE) - xi)}

    def y_peer(k):
        return {"space": s + 2 * SIDE * (lax.rem(yi + k, SIDE) - yi)}

    barrier = pltpu.get_barrier_semaphore()
    for k in range(1, octet):
        pl.semaphore_signal(barrier, inc=1, device_id=cube_peer(k)[1], device_id_type=MESH)
    for k in range(1, SIDE):
        pl.semaphore_signal(barrier, inc=1, device_id=x_peer(k), device_id_type=MESH)
        pl.semaphore_signal(barrier, inc=1, device_id=y_peer(k), device_id_type=MESH)

    other = s + 2 * core - 1
    has_other = jnp.logical_and(edge, jnp.logical_and(other >= 0, other < ns))

    @pl.when(has_other)
    def _():
        pl.semaphore_signal(barrier, inc=1, device_id={"space": other}, device_id_type=MESH)

    pl.semaphore_wait(barrier, octet - 1 + 2 * (SIDE - 1) + has_other.astype(jnp.int32))

    def send_o(k):
        return pltpu.make_async_remote_copy(
            src_ref=o_hbm, dst_ref=obuf.at[pl.ds(pl.multiple_of(r * nloc, nloc), nloc)],
            send_sem=o_send.at[k - 1], recv_sem=o_recv.at[k - 1],
            device_id={"rec": lax.rem(r + k, nr)}, device_id_type=MESH)

    def recv_o(k):
        src = lax.rem(r + nr - k, nr)
        return pltpu.make_async_remote_copy(
            src_ref=o_hbm, dst_ref=obuf.at[pl.ds(pl.multiple_of(src * nloc, nloc), nloc)],
            send_sem=o_send.at[k - 1], recv_sem=o_recv.at[k - 1],
            device_id={"rec": lax.rem(r + k, nr)}, device_id_type=MESH)

    def send_c(k, ch):
        to = lax.rem(r + k, nr)
        return pltpu.make_async_remote_copy(
            src_ref=c_hbm.at[:, pl.ds(pl.multiple_of(to * share + ch * CHUNK, CHUNK), CHUNK)],
            dst_ref=cbuf.at[pl.ds(pl.multiple_of(r * nloc, nloc), nloc), pl.ds(pl.multiple_of(ch * CHUNK, CHUNK), CHUNK)],
            send_sem=c_send.at[k - 1, ch], recv_sem=c_recv.at[k - 1, ch],
            device_id={"rec": to}, device_id_type=MESH)

    def recv_c(k, ch):
        src = lax.rem(r + nr - k, nr)
        return pltpu.make_async_remote_copy(
            src_ref=c_hbm.at[:, pl.ds(0, CHUNK)],
            dst_ref=cbuf.at[pl.ds(pl.multiple_of(src * nloc, nloc), nloc), pl.ds(pl.multiple_of(ch * CHUNK, CHUNK), CHUNK)],
            send_sem=c_send.at[k - 1, ch], recv_sem=c_recv.at[k - 1, ch],
            device_id={"rec": lax.rem(r + k, nr)}, device_id_type=MESH)

    for k in range(1, nr):
        send_o(k).start()

    tail = pltpu.make_async_remote_copy(
        src_ref=p_hbm.at[pl.ds(rows - HALO, HALO)], dst_ref=pbuf.at[pl.ds(0, HALO)],
        send_sem=h_send.at[0], recv_sem=h_recv.at[0],
        device_id={"space": lax.rem(s + 1, ns)}, device_id_type=MESH)
    head = pltpu.make_async_remote_copy(
        src_ref=p_hbm.at[pl.ds(0, HALO)], dst_ref=pbuf.at[pl.ds(share + HALO, HALO)],
        send_sem=h_send.at[1], recv_sem=h_recv.at[1],
        device_id={"space": lax.rem(s + ns - 1, ns)}, device_id_type=MESH)

    @pl.when(jnp.logical_and(first, has_right))
    def _():
        tail.start()

    @pl.when(jnp.logical_and(last, has_left))
    def _():
        head.start()

    for ch in range(nch):
        for k in (2, 1, 3):
            send_c(k, ch).start()

    @pl.when(jnp.logical_and(first, s == 0))
    def _():
        pbuf[pl.ds(0, HALO), :] = jnp.zeros((HALO, pbuf.shape[1]), BF16)

    @pl.when(jnp.logical_and(last, s == ns - 1))
    def _():
        pbuf[pl.ds(share + HALO, HALO), :] = jnp.zeros((HALO, pbuf.shape[1]), BF16)

    @pl.when(r > 0)
    def _():
        cp = pltpu.make_async_copy(
            p_hbm.at[pl.ds(pl.multiple_of(r * share - HALO, HALO), HALO)],
            pbuf.at[pl.ds(0, HALO)], local_sem.at[2])
        cp.start()
        cp.wait()

    @pl.when(r < nr - 1)
    def _():
        cp = pltpu.make_async_copy(
            p_hbm.at[pl.ds(pl.multiple_of((r + 1) * share, HALO), HALO)],
            pbuf.at[pl.ds(share + HALO, HALO)], local_sem.at[3])
        cp.start()
        cp.wait()

    @pl.when(jnp.logical_and(first, has_left))
    def _():
        tail.wait_recv()

    @pl.when(jnp.logical_and(last, has_right))
    def _():
        head.wait_recv()

    own_o.wait()
    for k in range(1, nr):
        recv_o(k).wait_recv()
    off = obuf[...]
    lane = lax.broadcasted_iota(jnp.int32, (B, B), 1)
    for t in range(3):
        sel[:, t * B:(t + 1) * B] = jnp.where(lane + (t * B - HALO) == off, 1.0, 0.0).astype(BF16)
    main.wait()
    g_ref[...] = jnp.zeros_like(g_ref)

    def block(p0):
        cols = cbuf[:, pl.ds(p0, B)]
        diag = dot(cols, sel[...], ((0,), (0,)))
        band = pltpu.roll(diag, 0, 1, stride=1, stride_axis=0)
        bh, bl = split(band)
        piece = pbuf[pl.ds(p0, 3 * B), :]
        sk = dot(bh, piece, ((1,), (0,))) + dot(bl, piece, ((1,), (0,)))
        hi, lo = split(sk)
        hl_ref[pl.ds(p0, B), 0:B] = hi
        hl_ref[pl.ds(p0, B), B:2 * B] = lo

    def step(i, _):
        base = pl.multiple_of(i * (UNROLL * B), UNROLL * B)
        for u in range(UNROLL):
            block(base + u * B)
        hl = hl_ref[pl.ds(base, UNROLL * B), :]
        g_ref[...] += dot(hl, hl, ((0,), (0,)))
        return 0

    def store_hl(ch):
        here = pl.ds(pl.multiple_of(ch * CHUNK, CHUNK), CHUNK)
        return pltpu.make_async_copy(hl_ref.at[here], hl_hbm.at[here], out_sem.at[ch])

    def chunk(ch, _):
        own_c(ch).wait()
        for k in (1, 3, 2):
            recv_c(k, ch).wait_recv()
        per = CHUNK // (UNROLL * B)
        lax.fori_loop(ch * per, (ch + 1) * per, step, 0)
        store_hl(ch).start()
        return 0

    lax.fori_loop(0, nch, chunk, 0)

    n = out_ref.shape[0]
    part = n // octet
    gsum[...] = (g_ref[0:n, 0:n] + g_ref[n:2 * n, n:2 * n]) + (g_ref[0:n, n:2 * n] + g_ref[n:2 * n, 0:n])

    def exchange(copies):
        for cp in copies:
            cp.start()
        for cp in copies:
            cp.wait_recv()

    def total(ref):
        acc = ref[0]
        for i in range(1, ref.shape[0]):
            acc = acc + ref[i]
        return acc

    scatter = []
    for k in range(1, octet):
        at, to = cube_peer(k)
        scatter.append(pltpu.make_async_remote_copy(
            src_ref=gsum.at[pl.ds(pl.multiple_of(at * part, part), part)], dst_ref=gpart.at[mine],
            send_sem=s_send.at[k - 1], recv_sem=s_recv.at[k - 1], device_id=to, device_id_type=MESH))
    gpart[mine] = gsum[pl.ds(pl.multiple_of(mine * part, part), part), :]
    exchange(scatter)
    gx[xi] = total(gpart)
    along_x = [pltpu.make_async_remote_copy(
        src_ref=gx.at[xi], dst_ref=gx.at[xi], send_sem=x_send.at[k - 1], recv_sem=x_recv.at[k - 1],
        device_id=x_peer(k), device_id_type=MESH) for k in range(1, SIDE)]
    exchange(along_x)
    gy[yi] = total(gx)
    along_y = [pltpu.make_async_remote_copy(
        src_ref=gy.at[yi], dst_ref=gy.at[yi], send_sem=y_send.at[k - 1], recv_sem=y_recv.at[k - 1],
        device_id=y_peer(k), device_id_type=MESH) for k in range(1, SIDE)]
    exchange(along_y)
    own = pl.ds(pl.multiple_of(mine * part, part), part)
    gall[own, :] = total(gy)
    gather = [pltpu.make_async_remote_copy(
        src_ref=gall.at[own], dst_ref=gall.at[own], send_sem=a_send.at[k - 1], recv_sem=a_recv.at[k - 1],
        device_id=cube_peer(k)[1], device_id_type=MESH) for k in range(1, octet)]
    exchange(gather)
    out_ref[...] = gall[...]
    for ch in range(nch):
        store_hl(ch).wait()
    for cp in scatter + along_x + along_y + gather:
        cp.wait_send()

    for k in range(1, nr):
        send_o(k).wait_send()
        for ch in range(nch):
            send_c(k, ch).wait_send()

    @pl.when(jnp.logical_and(first, has_right))
    def _():
        tail.wait_send()

    @pl.when(jnp.logical_and(last, has_left))
    def _():
        head.wait_send()


def eliminate(a, eye, n):
    nt = n // 8
    at = [a[8 * t:8 * t + 8] for t in range(nt)]
    it = [eye[8 * t:8 * t + 8] for t in range(nt)]
    sub = lax.broadcasted_iota(jnp.int32, (8, n), 0)

    def row(x, i):
        return jnp.broadcast_to(x[i:i + 1, :], (8, n))

    def col(x, j):
        return jnp.broadcast_to(x[:, j:j + 1], (8, n))

    for t0 in range(nt):
        j = 8 * t0
        head = [col(at[t0], j + i) for i in range(8)]
        piv = [[row(head[i], k) if k >= i else None for k in range(8)] for i in range(8)]
        inv, mult = [], [[None] * 8 for _ in range(8)]
        for i in range(8):
            inv.append(1.0 / piv[i][i])
            for k in range(i + 1, 8):
                mult[k][i] = piv[i][k] * inv[i]
            for k in range(i + 1, 8):
                for m in range(k, 8):
                    piv[k][m] = piv[k][m] - mult[k][i] * piv[i][m]
        ra = [row(at[t0], i) for i in range(8)]
        ri = [row(it[t0], i) for i in range(8)]
        for i in range(8):
            for k in range(i + 1, 8):
                ra[k] = ra[k] - mult[k][i] * ra[i]
                ri[k] = ri[k] - mult[k][i] * ri[i]
        sa = [x * v for x, v in zip(ra, inv)]
        si = [x * v for x, v in zip(ri, inv)]
        for t in range(t0, nt):
            c = head if t == t0 else [col(at[t], j + i) for i in range(8)]
            c = list(c)
            for i in range(8):
                for k in range(i + 1, 8):
                    c[k] = c[k] - mult[k][i] * c[i]
            for i in range(8):
                f = jnp.where(sub > i, c[i], 0.0) if t == t0 else c[i]
                at[t] = at[t] - f * sa[i]
                it[t] = it[t] - f * si[i]
    return jnp.concatenate(at, axis=0), jnp.concatenate(it, axis=0)


def factor_kernel(scale, hl_hbm, g_ref, q_ref, u_ref, w_ref, hl_ref, sem):
    n = g_ref.shape[0]
    tile = q_ref.shape[0]

    @pl.when(pl.program_id(0) == 0)
    def _():
        fetch = pltpu.make_async_copy(hl_hbm, hl_ref, sem)
        fetch.start()
        rowi = lax.broadcasted_iota(jnp.int32, (n, n), 0)
        lane = lax.broadcasted_iota(jnp.int32, (n, n), 1)
        eye = jnp.where(rowi == lane, 1.0, 0.0).astype(F32)
        a, linv = eliminate(g_ref[...], eye, n)
        diag = jnp.sum(jnp.where(rowi == lane, a, 0.0), axis=1, keepdims=True)
        rs = 1.0 / jnp.sqrt(diag)
        u_ref[...] = jnp.where(lane >= rowi, a, 0.0) * (rs * (1.0 / scale))
        linv = jnp.where(lane <= rowi, linv, 0.0) * (rs * scale)
        right = linv.T
        rh, rl = split(right)
        w_ref[0:n, 0:n] = rh
        w_ref[0:n, n:2 * n] = rl
        w_ref[n:2 * n, 0:n] = rh
        w_ref[n:2 * n, n:2 * n] = jnp.zeros((n, n), BF16)
        fetch.wait()

    here = pl.ds(pl.multiple_of(pl.program_id(0) * tile, tile), tile)
    out = dot(hl_ref[here, :], w_ref[...], ((1,), (0,)))
    q_ref[...] = out[:, :n] + out[:, n:]


def local(nr, ns, probes, band_coeffs, band_offsets):
    rows, k = probes.shape
    share = rows // nr
    nloc = band_coeffs.shape[0] * band_coeffs.shape[1]
    nall = nr * nloc
    nch = share // CHUNK
    octet = 2 * nr
    coeffs = band_coeffs.reshape(nloc, rows)
    offs = jnp.broadcast_to(band_offsets.reshape(nloc, 1), (nloc, B))
    hbm_spec = pl.BlockSpec(memory_space=pltpu.HBM)
    vmem_spec = pl.BlockSpec(memory_space=pltpu.VMEM)
    dma = pltpu.SemaphoreType.DMA
    hl, gram = pl.pallas_call(
        functools.partial(sketch_kernel, nr, ns),
        out_shape=(jax.ShapeDtypeStruct((share, 2 * k), BF16), jax.ShapeDtypeStruct((k, k), F32)),
        in_specs=[hbm_spec] * 3,
        out_specs=(hbm_spec, vmem_spec),
        scratch_shapes=[
            pltpu.VMEM((share, 2 * k), BF16),
            pltpu.VMEM((nall, share), BF16),
            pltpu.VMEM((nall, B), jnp.int32),
            pltpu.VMEM((nall, 3 * B), BF16),
            pltpu.VMEM((share + 2 * HALO, k), BF16),
            pltpu.VMEM((2 * k, 2 * k), F32),
            pltpu.VMEM((k, k), F32),
            pltpu.VMEM((octet, k // octet, k), F32),
            pltpu.VMEM((SIDE, k // octet, k), F32),
            pltpu.VMEM((SIDE, k // octet, k), F32),
            pltpu.VMEM((k, k), F32),
            dma((nr - 1, nch)), dma((nr - 1, nch)),
            dma((nr - 1,)), dma((nr - 1,)), dma((2,)), dma((2,)), dma((4,)), dma((nch,)), dma((nch,)),
            dma((octet - 1,)), dma((octet - 1,)), dma((SIDE - 1,)), dma((SIDE - 1,)),
            dma((SIDE - 1,)), dma((SIDE - 1,)), dma((octet - 1,)), dma((octet - 1,)),
        ],
        compiler_params=pltpu.CompilerParams(
            collective_id=0, has_side_effects=True, vmem_limit_bytes=48 << 20),
    )(coeffs, offs, probes)
    scale = math.sqrt(rows * ns)
    tile = 1024
    q, u = pl.pallas_call(
        functools.partial(factor_kernel, scale),
        grid=(share // tile,),
        out_shape=(jax.ShapeDtypeStruct((share, k), F32), jax.ShapeDtypeStruct((k, k), F32)),
        in_specs=[hbm_spec, vmem_spec],
        out_specs=(pl.BlockSpec((tile, k), lambda i: (i, 0)), pl.BlockSpec((k, k), lambda i: (0, 0))),
        scratch_shapes=[pltpu.VMEM((2 * k, 2 * k), BF16), pltpu.VMEM((share, 2 * k), BF16), dma],
        compiler_params=pltpu.CompilerParams(dimension_semantics=("arbitrary",), vmem_limit_bytes=32 << 20),
    )(hl, gram)
    return q, u


def solution(mesh):
    in_specs = (P("space", None), P("rec", None, "space"), P("rec", None))
    out_specs = (P(("space", "rec"), None), P())
    body = functools.partial(local, mesh.shape["rec"], mesh.shape["space"])
    return jax.shard_map(body, mesh=mesh, in_specs=in_specs, out_specs=out_specs, check_vma=False)
```

```python
import functools
import math

import jax
import jax.numpy as jnp
from jax import lax
from jax.experimental import pallas as pl
from jax.experimental.pallas import tpu as pltpu
from jax.sharding import PartitionSpec as P

HALO = 128
SIDE = 4
B = 128
CHUNK = 1024
UNROLL = 4
MESH = pl.DeviceIdType.MESH
F32 = jnp.float32
BF16 = jnp.bfloat16


def dot(a, b, dims):
    return lax.dot_general(a, b, (dims, ((), ())), preferred_element_type=F32)


def split(x):
    high = x.astype(BF16)
    low = (x - high.astype(F32)).astype(BF16)
    return high, low


def sketch_kernel(
    nr, ns, c_hbm, o_hbm, p_hbm, hl_hbm, out_ref,
    hl_ref, cbuf, obuf, sel, pbuf, g_ref, gsum, gpart, gx, gy, gall,
    c_send, c_recv, o_send, o_recv, h_send, h_recv, local_sem, own_sem, out_sem,
    s_send, s_recv, x_send, x_recv, y_send, y_recv, a_send, a_recv,
):
    r = lax.axis_index("rec")
    s = lax.axis_index("space")
    share = cbuf.shape[1]
    nloc = c_hbm.shape[0]
    rows = p_hbm.shape[0]
    nch = share // CHUNK
    first, last = r == 0, r == nr - 1
    has_left, has_right = s > 0, s < ns - 1
    edge = jnp.logical_or(first, last)

    main = pltpu.make_async_copy(
        p_hbm.at[pl.ds(pl.multiple_of(r * share, share), share)],
        pbuf.at[pl.ds(HALO, share)], local_sem.at[0])
    main.start()

    def own_c(ch):
        return pltpu.make_async_copy(
            c_hbm.at[:, pl.ds(pl.multiple_of(r * share + ch * CHUNK, CHUNK), CHUNK)],
            cbuf.at[pl.ds(pl.multiple_of(r * nloc, nloc), nloc), pl.ds(pl.multiple_of(ch * CHUNK, CHUNK), CHUNK)],
            own_sem.at[ch])

    for ch in range(nch):
        own_c(ch).start()
    own_o = pltpu.make_async_copy(
        o_hbm, obuf.at[pl.ds(pl.multiple_of(r * nloc, nloc), nloc)], local_sem.at[1])
    own_o.start()

    core = lax.rem(s, 2)
    xi = lax.rem(s // 2, SIDE)
    yi = s // (2 * SIDE)
    octet = 2 * nr
    mine = 2 * r + core

    def cube_peer(k):
        at = lax.rem(mine + k, octet)
        return at, {"rec": at // 2, "space": s - core + lax.rem(at, 2)}

    def x_peer(k):
        return {"space": s + 2 * (lax.rem(xi + k, SIDE) - xi)}

    def y_peer(k):
        return {"space": s + 2 * SIDE * (lax.rem(yi + k, SIDE) - yi)}

    barrier = pltpu.get_barrier_semaphore()
    for k in range(1, octet):
        pl.semaphore_signal(barrier, inc=1, device_id=cube_peer(k)[1], device_id_type=MESH)
    for k in range(1, SIDE):
        pl.semaphore_signal(barrier, inc=1, device_id=x_peer(k), device_id_type=MESH)
        pl.semaphore_signal(barrier, inc=1, device_id=y_peer(k), device_id_type=MESH)

    other = s + 2 * core - 1
    has_other = jnp.logical_and(edge, jnp.logical_and(other >= 0, other < ns))

    @pl.when(has_other)
    def _():
        pl.semaphore_signal(barrier, inc=1, device_id={"space": other}, device_id_type=MESH)

    pl.semaphore_wait(barrier, octet - 1 + 2 * (SIDE - 1) + has_other.astype(jnp.int32))

    def send_o(k):
        return pltpu.make_async_remote_copy(
            src_ref=o_hbm, dst_ref=obuf.at[pl.ds(pl.multiple_of(r * nloc, nloc), nloc)],
            send_sem=o_send.at[k - 1], recv_sem=o_recv.at[k - 1],
            device_id={"rec": lax.rem(r + k, nr)}, device_id_type=MESH)

    def recv_o(k):
        src = lax.rem(r + nr - k, nr)
        return pltpu.make_async_remote_copy(
            src_ref=o_hbm, dst_ref=obuf.at[pl.ds(pl.multiple_of(src * nloc, nloc), nloc)],
            send_sem=o_send.at[k - 1], recv_sem=o_recv.at[k - 1],
            device_id={"rec": lax.rem(r + k, nr)}, device_id_type=MESH)

    def send_c(k, ch):
        to = lax.rem(r + k, nr)
        return pltpu.make_async_remote_copy(
            src_ref=c_hbm.at[:, pl.ds(pl.multiple_of(to * share + ch * CHUNK, CHUNK), CHUNK)],
            dst_ref=cbuf.at[pl.ds(pl.multiple_of(r * nloc, nloc), nloc), pl.ds(pl.multiple_of(ch * CHUNK, CHUNK), CHUNK)],
            send_sem=c_send.at[k - 1, ch], recv_sem=c_recv.at[k - 1, ch],
            device_id={"rec": to}, device_id_type=MESH)

    def recv_c(k, ch):
        src = lax.rem(r + nr - k, nr)
        return pltpu.make_async_remote_copy(
            src_ref=c_hbm.at[:, pl.ds(0, CHUNK)],
            dst_ref=cbuf.at[pl.ds(pl.multiple_of(src * nloc, nloc), nloc), pl.ds(pl.multiple_of(ch * CHUNK, CHUNK), CHUNK)],
            send_sem=c_send.at[k - 1, ch], recv_sem=c_recv.at[k - 1, ch],
            device_id={"rec": lax.rem(r + k, nr)}, device_id_type=MESH)

    for k in range(1, nr):
        send_o(k).start()

    tail = pltpu.make_async_remote_copy(
        src_ref=p_hbm.at[pl.ds(rows - HALO, HALO)], dst_ref=pbuf.at[pl.ds(0, HALO)],
        send_sem=h_send.at[0], recv_sem=h_recv.at[0],
        device_id={"space": lax.rem(s + 1, ns)}, device_id_type=MESH)
    head = pltpu.make_async_remote_copy(
        src_ref=p_hbm.at[pl.ds(0, HALO)], dst_ref=pbuf.at[pl.ds(share + HALO, HALO)],
        send_sem=h_send.at[1], recv_sem=h_recv.at[1],
        device_id={"space": lax.rem(s + ns - 1, ns)}, device_id_type=MESH)

    @pl.when(jnp.logical_and(first, has_right))
    def _():
        tail.start()

    @pl.when(jnp.logical_and(last, has_left))
    def _():
        head.start()

    for ch in range(nch):
        for k in (2, 1, 3):
            send_c(k, ch).start()

    @pl.when(jnp.logical_and(first, s == 0))
    def _():
        pbuf[pl.ds(0, HALO), :] = jnp.zeros((HALO, pbuf.shape[1]), BF16)

    @pl.when(jnp.logical_and(last, s == ns - 1))
    def _():
        pbuf[pl.ds(share + HALO, HALO), :] = jnp.zeros((HALO, pbuf.shape[1]), BF16)

    @pl.when(r > 0)
    def _():
        cp = pltpu.make_async_copy(
            p_hbm.at[pl.ds(pl.multiple_of(r * share - HALO, HALO), HALO)],
            pbuf.at[pl.ds(0, HALO)], local_sem.at[2])
        cp.start()
        cp.wait()

    @pl.when(r < nr - 1)
    def _():
        cp = pltpu.make_async_copy(
            p_hbm.at[pl.ds(pl.multiple_of((r + 1) * share, HALO), HALO)],
            pbuf.at[pl.ds(share + HALO, HALO)], local_sem.at[3])
        cp.start()
        cp.wait()

    @pl.when(jnp.logical_and(first, has_left))
    def _():
        tail.wait_recv()

    @pl.when(jnp.logical_and(last, has_right))
    def _():
        head.wait_recv()

    own_o.wait()
    for k in range(1, nr):
        recv_o(k).wait_recv()
    off = obuf[...]
    lane = lax.broadcasted_iota(jnp.int32, (B, B), 1)
    for t in range(3):
        sel[:, t * B:(t + 1) * B] = jnp.where(lane + (t * B - HALO) == off, 1.0, 0.0).astype(BF16)
    main.wait()
    g_ref[...] = jnp.zeros_like(g_ref)

    def block(p0):
        cols = cbuf[:, pl.ds(p0, B)]
        diag = dot(cols, sel[...], ((0,), (0,)))
        band = pltpu.roll(diag, 0, 1, stride=1, stride_axis=0)
        bh, bl = split(band)
        piece = pbuf[pl.ds(p0, 3 * B), :]
        both = dot(jnp.concatenate([bh, bl], axis=0), piece, ((1,), (0,)))
        sk = both[:B] + both[B:]
        hi, lo = split(sk)
        hl_ref[pl.ds(p0, B), 0:B] = hi
        hl_ref[pl.ds(p0, B), B:2 * B] = lo

    def step(i, _):
        base = pl.multiple_of(i * (UNROLL * B), UNROLL * B)
        for u in range(UNROLL):
            block(base + u * B)
        hl = hl_ref[pl.ds(base, UNROLL * B), :]
        g_ref[...] += dot(hl, hl, ((0,), (0,)))
        return 0

    def store_hl(ch):
        here = pl.ds(pl.multiple_of(ch * CHUNK, CHUNK), CHUNK)
        return pltpu.make_async_copy(hl_ref.at[here], hl_hbm.at[here], out_sem.at[ch])

    def chunk(ch, _):
        own_c(ch).wait()
        for k in (1, 3, 2):
            recv_c(k, ch).wait_recv()
        per = CHUNK // (UNROLL * B)
        lax.fori_loop(ch * per, (ch + 1) * per, step, 0)
        store_hl(ch).start()
        return 0

    lax.fori_loop(0, nch, chunk, 0)

    n = out_ref.shape[0]
    part = n // octet
    gsum[...] = (g_ref[0:n, 0:n] + g_ref[n:2 * n, n:2 * n]) + (g_ref[0:n, n:2 * n] + g_ref[n:2 * n, 0:n])

    def exchange(copies):
        for cp in copies:
            cp.start()
        for cp in copies:
            cp.wait_recv()

    def total(ref):
        acc = ref[0]
        for i in range(1, ref.shape[0]):
            acc = acc + ref[i]
        return acc

    scatter = []
    for k in range(1, octet):
        at, to = cube_peer(k)
        scatter.append(pltpu.make_async_remote_copy(
            src_ref=gsum.at[pl.ds(pl.multiple_of(at * part, part), part)], dst_ref=gpart.at[mine],
            send_sem=s_send.at[k - 1], recv_sem=s_recv.at[k - 1], device_id=to, device_id_type=MESH))
    gpart[mine] = gsum[pl.ds(pl.multiple_of(mine * part, part), part), :]
    exchange(scatter)
    gx[xi] = total(gpart)
    along_x = [pltpu.make_async_remote_copy(
        src_ref=gx.at[xi], dst_ref=gx.at[xi], send_sem=x_send.at[k - 1], recv_sem=x_recv.at[k - 1],
        device_id=x_peer(k), device_id_type=MESH) for k in range(1, SIDE)]
    exchange(along_x)
    gy[yi] = total(gx)
    along_y = [pltpu.make_async_remote_copy(
        src_ref=gy.at[yi], dst_ref=gy.at[yi], send_sem=y_send.at[k - 1], recv_sem=y_recv.at[k - 1],
        device_id=y_peer(k), device_id_type=MESH) for k in range(1, SIDE)]
    exchange(along_y)
    own = pl.ds(pl.multiple_of(mine * part, part), part)
    gall[own, :] = total(gy)
    gather = [pltpu.make_async_remote_copy(
        src_ref=gall.at[own], dst_ref=gall.at[own], send_sem=a_send.at[k - 1], recv_sem=a_recv.at[k - 1],
        device_id=cube_peer(k)[1], device_id_type=MESH) for k in range(1, octet)]
    exchange(gather)
    out_ref[...] = gall[...]
    for ch in range(nch):
        store_hl(ch).wait()
    for cp in scatter + along_x + along_y + gather:
        cp.wait_send()

    for k in range(1, nr):
        send_o(k).wait_send()
        for ch in range(nch):
            send_c(k, ch).wait_send()

    @pl.when(jnp.logical_and(first, has_right))
    def _():
        tail.wait_send()

    @pl.when(jnp.logical_and(last, has_left))
    def _():
        head.wait_send()


def eliminate(a, eye, n):
    nt = n // 8
    at = [a[8 * t:8 * t + 8] for t in range(nt)]
    it = [eye[8 * t:8 * t + 8] for t in range(nt)]
    sub = lax.broadcasted_iota(jnp.int32, (8, n), 0)

    def row(x, i):
        return jnp.broadcast_to(x[i:i + 1, :], (8, n))

    def col(x, j):
        return jnp.broadcast_to(x[:, j:j + 1], (8, n))

    for t0 in range(nt):
        j = 8 * t0
        head = [col(at[t0], j + i) for i in range(8)]
        piv = [[row(head[i], k) if k >= i else None for k in range(8)] for i in range(8)]
        inv, mult = [], [[None] * 8 for _ in range(8)]
        for i in range(8):
            inv.append(1.0 / piv[i][i])
            for k in range(i + 1, 8):
                mult[k][i] = piv[i][k] * inv[i]
            for k in range(i + 1, 8):
                for m in range(k, 8):
                    piv[k][m] = piv[k][m] - mult[k][i] * piv[i][m]
        ra = [row(at[t0], i) for i in range(8)]
        ri = [row(it[t0], i) for i in range(8)]
        for i in range(8):
            for k in range(i + 1, 8):
                ra[k] = ra[k] - mult[k][i] * ra[i]
                ri[k] = ri[k] - mult[k][i] * ri[i]
        sa = [x * v for x, v in zip(ra, inv)]
        si = [x * v for x, v in zip(ri, inv)]
        for t in range(t0, nt):
            c = head if t == t0 else [col(at[t], j + i) for i in range(8)]
            c = list(c)
            for i in range(8):
                for k in range(i + 1, 8):
                    c[k] = c[k] - mult[k][i] * c[i]
            for i in range(8):
                f = jnp.where(sub > i, c[i], 0.0) if t == t0 else c[i]
                at[t] = at[t] - f * sa[i]
                it[t] = it[t] - f * si[i]
    return jnp.concatenate(at, axis=0), jnp.concatenate(it, axis=0)


def factor_kernel(scale, hl_hbm, g_ref, q_ref, u_ref, w_ref, hl_ref, sem):
    n = g_ref.shape[0]
    tile = q_ref.shape[0]

    @pl.when(pl.program_id(0) == 0)
    def _():
        fetch = pltpu.make_async_copy(hl_hbm, hl_ref, sem)
        fetch.start()
        rowi = lax.broadcasted_iota(jnp.int32, (n, n), 0)
        lane = lax.broadcasted_iota(jnp.int32, (n, n), 1)
        eye = jnp.where(rowi == lane, 1.0, 0.0).astype(F32)
        a, linv = eliminate(g_ref[...], eye, n)
        diag = jnp.sum(jnp.where(rowi == lane, a, 0.0), axis=1, keepdims=True)
        rs = 1.0 / jnp.sqrt(diag)
        u_ref[...] = jnp.where(lane >= rowi, a, 0.0) * (rs * (1.0 / scale))
        linv = jnp.where(lane <= rowi, linv, 0.0) * (rs * scale)
        right = linv.T
        rh, rl = split(right)
        w_ref[0:n, 0:n] = rh
        w_ref[0:n, n:2 * n] = rl
        w_ref[n:2 * n, 0:n] = rh
        w_ref[n:2 * n, n:2 * n] = jnp.zeros((n, n), BF16)
        fetch.wait()

    here = pl.ds(pl.multiple_of(pl.program_id(0) * tile, tile), tile)
    out = dot(hl_ref[here, :], w_ref[...], ((1,), (0,)))
    q_ref[...] = out[:, :n] + out[:, n:]


def local(nr, ns, probes, band_coeffs, band_offsets):
    rows, k = probes.shape
    share = rows // nr
    nloc = band_coeffs.shape[0] * band_coeffs.shape[1]
    nall = nr * nloc
    nch = share // CHUNK
    octet = 2 * nr
    coeffs = pltpu.with_memory_space_constraint(band_coeffs.reshape(nloc, rows), pltpu.HBM)
    offs = jnp.broadcast_to(band_offsets.reshape(nloc, 1), (nloc, B))
    hbm_spec = pl.BlockSpec(memory_space=pltpu.HBM)
    vmem_spec = pl.BlockSpec(memory_space=pltpu.VMEM)
    dma = pltpu.SemaphoreType.DMA
    hl, gram = pl.pallas_call(
        functools.partial(sketch_kernel, nr, ns),
        out_shape=(jax.ShapeDtypeStruct((share, 2 * k), BF16), jax.ShapeDtypeStruct((k, k), F32)),
        in_specs=[hbm_spec] * 3,
        out_specs=(hbm_spec, vmem_spec),
        scratch_shapes=[
            pltpu.VMEM((share, 2 * k), BF16),
            pltpu.VMEM((nall, share), BF16),
            pltpu.VMEM((nall, B), jnp.int32),
            pltpu.VMEM((nall, 3 * B), BF16),
            pltpu.VMEM((share + 2 * HALO, k), BF16),
            pltpu.VMEM((2 * k, 2 * k), F32),
            pltpu.VMEM((k, k), F32),
            pltpu.VMEM((octet, k // octet, k), F32),
            pltpu.VMEM((SIDE, k // octet, k), F32),
            pltpu.VMEM((SIDE, k // octet, k), F32),
            pltpu.VMEM((k, k), F32),
            dma((nr - 1, nch)), dma((nr - 1, nch)),
            dma((nr - 1,)), dma((nr - 1,)), dma((2,)), dma((2,)), dma((4,)), dma((nch,)), dma((nch,)),
            dma((octet - 1,)), dma((octet - 1,)), dma((SIDE - 1,)), dma((SIDE - 1,)),
            dma((SIDE - 1,)), dma((SIDE - 1,)), dma((octet - 1,)), dma((octet - 1,)),
        ],
        compiler_params=pltpu.CompilerParams(
            collective_id=0, has_side_effects=True, vmem_limit_bytes=48 << 20),
    )(coeffs, offs, pltpu.with_memory_space_constraint(probes, pltpu.HBM))
    scale = math.sqrt(rows * ns)
    tile = 1024
    q, u = pl.pallas_call(
        functools.partial(factor_kernel, scale),
        grid=(share // tile,),
        out_shape=(jax.ShapeDtypeStruct((share, k), F32), jax.ShapeDtypeStruct((k, k), F32)),
        in_specs=[hbm_spec, vmem_spec],
        out_specs=(pl.BlockSpec((tile, k), lambda i: (i, 0)), pl.BlockSpec((k, k), lambda i: (0, 0))),
        scratch_shapes=[pltpu.VMEM((2 * k, 2 * k), BF16), pltpu.VMEM((share, 2 * k), BF16), dma],
        compiler_params=pltpu.CompilerParams(dimension_semantics=("arbitrary",), vmem_limit_bytes=32 << 20),
    )(hl, gram)
    return q, u


def solution(mesh):
    in_specs = (P("space", None), P("rec", None, "space"), P("rec", None))
    out_specs = (P(("space", "rec"), None), P())
    body = functools.partial(local, mesh.shape["rec"], mesh.shape["space"])
    return jax.shard_map(body, mesh=mesh, in_specs=in_specs, out_specs=out_specs, check_vma=False)
```

```python
import functools
import math

import jax
import jax.numpy as jnp
from jax import lax
from jax.experimental import pallas as pl
from jax.experimental.pallas import tpu as pltpu
from jax.sharding import PartitionSpec as P

HALO = 128
SIDE = 4
B = 128
CHUNK = 1024
UNROLL = 4
MESH = pl.DeviceIdType.MESH
F32 = jnp.float32
BF16 = jnp.bfloat16


def dot(a, b, dims):
    return lax.dot_general(a, b, (dims, ((), ())), preferred_element_type=F32)


def split(x):
    high = x.astype(BF16)
    low = (x - high.astype(F32)).astype(BF16)
    return high, low


def sketch_kernel(
    nr, ns, c_hbm, o_hbm, p_hbm, hl_hbm, out_ref,
    hl_ref, cbuf, obuf, sel, pbuf, g_ref, gsum, gpart, gx, gy, gall,
    c_send, c_recv, o_send, o_recv, h_send, h_recv, local_sem, own_sem, out_sem,
    s_send, s_recv, x_send, x_recv, y_send, y_recv, a_send, a_recv,
):
    r = lax.axis_index("rec")
    s = lax.axis_index("space")
    share = cbuf.shape[1]
    nloc = c_hbm.shape[0]
    rows = p_hbm.shape[0]
    nch = share // CHUNK
    first, last = r == 0, r == nr - 1
    has_left, has_right = s > 0, s < ns - 1
    edge = jnp.logical_or(first, last)

    main = pltpu.make_async_copy(
        p_hbm.at[pl.ds(pl.multiple_of(r * share, share), share)],
        pbuf.at[pl.ds(HALO, share)], local_sem.at[0])
    main.start()

    def own_c(ch):
        return pltpu.make_async_copy(
            c_hbm.at[:, pl.ds(pl.multiple_of(r * share + ch * CHUNK, CHUNK), CHUNK)],
            cbuf.at[pl.ds(pl.multiple_of(r * nloc, nloc), nloc), pl.ds(pl.multiple_of(ch * CHUNK, CHUNK), CHUNK)],
            own_sem.at[ch])

    for ch in range(nch):
        own_c(ch).start()
    own_o = pltpu.make_async_copy(
        o_hbm, obuf.at[pl.ds(pl.multiple_of(r * nloc, nloc), nloc)], local_sem.at[1])
    own_o.start()

    core = lax.rem(s, 2)
    xi = lax.rem(s // 2, SIDE)
    yi = s // (2 * SIDE)
    octet = 2 * nr
    mine = 2 * r + core

    def cube_peer(k):
        at = lax.rem(mine + k, octet)
        return at, {"rec": at // 2, "space": s - core + lax.rem(at, 2)}

    def x_peer(k):
        return {"space": s + 2 * (lax.rem(xi + k, SIDE) - xi)}

    def y_peer(k):
        return {"space": s + 2 * SIDE * (lax.rem(yi + k, SIDE) - yi)}

    barrier = pltpu.get_barrier_semaphore()
    for k in range(1, octet):
        pl.semaphore_signal(barrier, inc=1, device_id=cube_peer(k)[1], device_id_type=MESH)
    for k in range(1, SIDE):
        pl.semaphore_signal(barrier, inc=1, device_id=x_peer(k), device_id_type=MESH)
        pl.semaphore_signal(barrier, inc=1, device_id=y_peer(k), device_id_type=MESH)

    other = s + 2 * core - 1
    has_other = jnp.logical_and(edge, jnp.logical_and(other >= 0, other < ns))

    @pl.when(has_other)
    def _():
        pl.semaphore_signal(barrier, inc=1, device_id={"space": other}, device_id_type=MESH)

    pl.semaphore_wait(barrier, octet - 1 + 2 * (SIDE - 1) + has_other.astype(jnp.int32))

    def send_o(k):
        return pltpu.make_async_remote_copy(
            src_ref=o_hbm, dst_ref=obuf.at[pl.ds(pl.multiple_of(r * nloc, nloc), nloc)],
            send_sem=o_send.at[k - 1], recv_sem=o_recv.at[k - 1],
            device_id={"rec": lax.rem(r + k, nr)}, device_id_type=MESH)

    def recv_o(k):
        src = lax.rem(r + nr - k, nr)
        return pltpu.make_async_remote_copy(
            src_ref=o_hbm, dst_ref=obuf.at[pl.ds(pl.multiple_of(src * nloc, nloc), nloc)],
            send_sem=o_send.at[k - 1], recv_sem=o_recv.at[k - 1],
            device_id={"rec": lax.rem(r + k, nr)}, device_id_type=MESH)

    def send_c(k, ch):
        to = lax.rem(r + k, nr)
        return pltpu.make_async_remote_copy(
            src_ref=c_hbm.at[:, pl.ds(pl.multiple_of(to * share + ch * CHUNK, CHUNK), CHUNK)],
            dst_ref=cbuf.at[pl.ds(pl.multiple_of(r * nloc, nloc), nloc), pl.ds(pl.multiple_of(ch * CHUNK, CHUNK), CHUNK)],
            send_sem=c_send.at[k - 1, ch], recv_sem=c_recv.at[k - 1, ch],
            device_id={"rec": to}, device_id_type=MESH)

    def recv_c(k, ch):
        src = lax.rem(r + nr - k, nr)
        return pltpu.make_async_remote_copy(
            src_ref=c_hbm.at[:, pl.ds(0, CHUNK)],
            dst_ref=cbuf.at[pl.ds(pl.multiple_of(src * nloc, nloc), nloc), pl.ds(pl.multiple_of(ch * CHUNK, CHUNK), CHUNK)],
            send_sem=c_send.at[k - 1, ch], recv_sem=c_recv.at[k - 1, ch],
            device_id={"rec": lax.rem(r + k, nr)}, device_id_type=MESH)

    for k in range(1, nr):
        send_o(k).start()

    tail = pltpu.make_async_remote_copy(
        src_ref=p_hbm.at[pl.ds(rows - HALO, HALO)], dst_ref=pbuf.at[pl.ds(0, HALO)],
        send_sem=h_send.at[0], recv_sem=h_recv.at[0],
        device_id={"space": lax.rem(s + 1, ns)}, device_id_type=MESH)
    head = pltpu.make_async_remote_copy(
        src_ref=p_hbm.at[pl.ds(0, HALO)], dst_ref=pbuf.at[pl.ds(share + HALO, HALO)],
        send_sem=h_send.at[1], recv_sem=h_recv.at[1],
        device_id={"space": lax.rem(s + ns - 1, ns)}, device_id_type=MESH)

    @pl.when(jnp.logical_and(first, has_right))
    def _():
        tail.start()

    @pl.when(jnp.logical_and(last, has_left))
    def _():
        head.start()

    for ch in range(nch):
        for k in (2, 1, 3):
            send_c(k, ch).start()

    @pl.when(jnp.logical_and(first, s == 0))
    def _():
        pbuf[pl.ds(0, HALO), :] = jnp.zeros((HALO, pbuf.shape[1]), BF16)

    @pl.when(jnp.logical_and(last, s == ns - 1))
    def _():
        pbuf[pl.ds(share + HALO, HALO), :] = jnp.zeros((HALO, pbuf.shape[1]), BF16)

    @pl.when(r > 0)
    def _():
        cp = pltpu.make_async_copy(
            p_hbm.at[pl.ds(pl.multiple_of(r * share - HALO, HALO), HALO)],
            pbuf.at[pl.ds(0, HALO)], local_sem.at[2])
        cp.start()
        cp.wait()

    @pl.when(r < nr - 1)
    def _():
        cp = pltpu.make_async_copy(
            p_hbm.at[pl.ds(pl.multiple_of((r + 1) * share, HALO), HALO)],
            pbuf.at[pl.ds(share + HALO, HALO)], local_sem.at[3])
        cp.start()
        cp.wait()

    @pl.when(jnp.logical_and(first, has_left))
    def _():
        tail.wait_recv()

    @pl.when(jnp.logical_and(last, has_right))
    def _():
        head.wait_recv()

    own_o.wait()
    for k in range(1, nr):
        recv_o(k).wait_recv()
    off = obuf[...]
    lane = lax.broadcasted_iota(jnp.int32, (B, B), 1)
    for t in range(3):
        sel[:, t * B:(t + 1) * B] = jnp.where(lane + (t * B - HALO) == off, 1.0, 0.0).astype(BF16)
    main.wait()
    g_ref[...] = jnp.zeros_like(g_ref)

    def step(i, _):
        base = pl.multiple_of(i * (UNROLL * B), UNROLL * B)
        cols = cbuf[:, pl.ds(base, UNROLL * B)]
        diag = dot(cols, sel[...], ((0,), (0,)))
        bands = [pltpu.roll(diag[u * B:(u + 1) * B], 0, 1, stride=1, stride_axis=0) for u in range(UNROLL)]
        rows_of = []
        for u in range(UNROLL):
            bh, bl = split(bands[u])
            piece = pbuf[pl.ds(base + u * B, 3 * B), :]
            both = dot(jnp.concatenate([bh, bl], axis=0), piece, ((1,), (0,)))
            rows_of.append(both[:B] + both[B:])
        hi, lo = split(jnp.concatenate(rows_of, axis=0))
        hl = jnp.concatenate([hi, lo], axis=1)
        hl_ref[pl.ds(base, UNROLL * B), :] = hl
        g_ref[...] += dot(hl, hl, ((0,), (0,)))
        return 0

    def store_hl(ch):
        here = pl.ds(pl.multiple_of(ch * CHUNK, CHUNK), CHUNK)
        return pltpu.make_async_copy(hl_ref.at[here], hl_hbm.at[here], out_sem.at[ch])

    def chunk(ch, _):
        own_c(ch).wait()
        for k in (1, 3, 2):
            recv_c(k, ch).wait_recv()
        per = CHUNK // (UNROLL * B)
        lax.fori_loop(ch * per, (ch + 1) * per, step, 0)
        store_hl(ch).start()
        return 0

    lax.fori_loop(0, nch, chunk, 0)

    n = out_ref.shape[0]
    part = n // octet
    gsum[...] = (g_ref[0:n, 0:n] + g_ref[n:2 * n, n:2 * n]) + (g_ref[0:n, n:2 * n] + g_ref[n:2 * n, 0:n])

    def exchange(copies):
        for cp in copies:
            cp.start()
        for cp in copies:
            cp.wait_recv()

    def total(ref):
        acc = ref[0]
        for i in range(1, ref.shape[0]):
            acc = acc + ref[i]
        return acc

    scatter = []
    for k in range(1, octet):
        at, to = cube_peer(k)
        scatter.append(pltpu.make_async_remote_copy(
            src_ref=gsum.at[pl.ds(pl.multiple_of(at * part, part), part)], dst_ref=gpart.at[mine],
            send_sem=s_send.at[k - 1], recv_sem=s_recv.at[k - 1], device_id=to, device_id_type=MESH))
    gpart[mine] = gsum[pl.ds(pl.multiple_of(mine * part, part), part), :]
    exchange(scatter)
    gx[xi] = total(gpart)
    along_x = [pltpu.make_async_remote_copy(
        src_ref=gx.at[xi], dst_ref=gx.at[xi], send_sem=x_send.at[k - 1], recv_sem=x_recv.at[k - 1],
        device_id=x_peer(k), device_id_type=MESH) for k in range(1, SIDE)]
    exchange(along_x)
    gy[yi] = total(gx)
    along_y = [pltpu.make_async_remote_copy(
        src_ref=gy.at[yi], dst_ref=gy.at[yi], send_sem=y_send.at[k - 1], recv_sem=y_recv.at[k - 1],
        device_id=y_peer(k), device_id_type=MESH) for k in range(1, SIDE)]
    exchange(along_y)
    own = pl.ds(pl.multiple_of(mine * part, part), part)
    gall[own, :] = total(gy)
    gather = [pltpu.make_async_remote_copy(
        src_ref=gall.at[own], dst_ref=gall.at[own], send_sem=a_send.at[k - 1], recv_sem=a_recv.at[k - 1],
        device_id=cube_peer(k)[1], device_id_type=MESH) for k in range(1, octet)]
    exchange(gather)
    out_ref[...] = gall[...]
    for ch in range(nch):
        store_hl(ch).wait()
    for cp in scatter + along_x + along_y + gather:
        cp.wait_send()

    for k in range(1, nr):
        send_o(k).wait_send()
        for ch in range(nch):
            send_c(k, ch).wait_send()

    @pl.when(jnp.logical_and(first, has_right))
    def _():
        tail.wait_send()

    @pl.when(jnp.logical_and(last, has_left))
    def _():
        head.wait_send()


def eliminate(a, eye, n):
    nt = n // 8
    at = [a[8 * t:8 * t + 8] for t in range(nt)]
    it = [eye[8 * t:8 * t + 8] for t in range(nt)]
    sub = lax.broadcasted_iota(jnp.int32, (8, n), 0)

    def row(x, i):
        return jnp.broadcast_to(x[i:i + 1, :], (8, n))

    def col(x, j):
        return jnp.broadcast_to(x[:, j:j + 1], (8, n))

    for t0 in range(nt):
        j = 8 * t0
        head = [col(at[t0], j + i) for i in range(8)]
        piv = [[row(head[i], k) if k >= i else None for k in range(8)] for i in range(8)]
        inv, mult = [], [[None] * 8 for _ in range(8)]
        for i in range(8):
            inv.append(1.0 / piv[i][i])
            for k in range(i + 1, 8):
                mult[k][i] = piv[i][k] * inv[i]
            for k in range(i + 1, 8):
                for m in range(k, 8):
                    piv[k][m] = piv[k][m] - mult[k][i] * piv[i][m]
        ra = [row(at[t0], i) for i in range(8)]
        ri = [row(it[t0], i) for i in range(8)]
        for i in range(8):
            for k in range(i + 1, 8):
                ra[k] = ra[k] - mult[k][i] * ra[i]
                ri[k] = ri[k] - mult[k][i] * ri[i]
        sa = [x * v for x, v in zip(ra, inv)]
        si = [x * v for x, v in zip(ri, inv)]
        for t in range(t0, nt):
            c = head if t == t0 else [col(at[t], j + i) for i in range(8)]
            c = list(c)
            for i in range(8):
                for k in range(i + 1, 8):
                    c[k] = c[k] - mult[k][i] * c[i]
            for i in range(8):
                f = jnp.where(sub > i, c[i], 0.0) if t == t0 else c[i]
                at[t] = at[t] - f * sa[i]
                it[t] = it[t] - f * si[i]
    return jnp.concatenate(at, axis=0), jnp.concatenate(it, axis=0)


def factor_kernel(scale, hl_hbm, g_ref, q_ref, u_ref, w_ref, hl_ref, sem):
    n = g_ref.shape[0]
    tile = q_ref.shape[0]

    @pl.when(pl.program_id(0) == 0)
    def _():
        fetch = pltpu.make_async_copy(hl_hbm, hl_ref, sem)
        fetch.start()
        rowi = lax.broadcasted_iota(jnp.int32, (n, n), 0)
        lane = lax.broadcasted_iota(jnp.int32, (n, n), 1)
        eye = jnp.where(rowi == lane, 1.0, 0.0).astype(F32)
        a, linv = eliminate(g_ref[...], eye, n)
        diag = jnp.sum(jnp.where(rowi == lane, a, 0.0), axis=1, keepdims=True)
        rs = 1.0 / jnp.sqrt(diag)
        u_ref[...] = jnp.where(lane >= rowi, a, 0.0) * (rs * (1.0 / scale))
        linv = jnp.where(lane <= rowi, linv, 0.0) * (rs * scale)
        right = linv.T
        rh, rl = split(right)
        w_ref[0:n, 0:n] = rh
        w_ref[0:n, n:2 * n] = rl
        w_ref[n:2 * n, 0:n] = rh
        w_ref[n:2 * n, n:2 * n] = jnp.zeros((n, n), BF16)
        fetch.wait()

    here = pl.ds(pl.multiple_of(pl.program_id(0) * tile, tile), tile)
    out = dot(hl_ref[here, :], w_ref[...], ((1,), (0,)))
    q_ref[...] = out[:, :n] + out[:, n:]


def local(nr, ns, probes, band_coeffs, band_offsets):
    rows, k = probes.shape
    share = rows // nr
    nloc = band_coeffs.shape[0] * band_coeffs.shape[1]
    nall = nr * nloc
    nch = share // CHUNK
    octet = 2 * nr
    coeffs = pltpu.with_memory_space_constraint(band_coeffs.reshape(nloc, rows), pltpu.HBM)
    offs = jnp.broadcast_to(band_offsets.reshape(nloc, 1), (nloc, B))
    hbm_spec = pl.BlockSpec(memory_space=pltpu.HBM)
    vmem_spec = pl.BlockSpec(memory_space=pltpu.VMEM)
    dma = pltpu.SemaphoreType.DMA
    hl, gram = pl.pallas_call(
        functools.partial(sketch_kernel, nr, ns),
        out_shape=(jax.ShapeDtypeStruct((share, 2 * k), BF16), jax.ShapeDtypeStruct((k, k), F32)),
        in_specs=[hbm_spec] * 3,
        out_specs=(hbm_spec, vmem_spec),
        scratch_shapes=[
            pltpu.VMEM((share, 2 * k), BF16),
            pltpu.VMEM((nall, share), BF16),
            pltpu.VMEM((nall, B), jnp.int32),
            pltpu.VMEM((nall, 3 * B), BF16),
            pltpu.VMEM((share + 2 * HALO, k), BF16),
            pltpu.VMEM((2 * k, 2 * k), F32),
            pltpu.VMEM((k, k), F32),
            pltpu.VMEM((octet, k // octet, k), F32),
            pltpu.VMEM((SIDE, k // octet, k), F32),
            pltpu.VMEM((SIDE, k // octet, k), F32),
            pltpu.VMEM((k, k), F32),
            dma((nr - 1, nch)), dma((nr - 1, nch)),
            dma((nr - 1,)), dma((nr - 1,)), dma((2,)), dma((2,)), dma((4,)), dma((nch,)), dma((nch,)),
            dma((octet - 1,)), dma((octet - 1,)), dma((SIDE - 1,)), dma((SIDE - 1,)),
            dma((SIDE - 1,)), dma((SIDE - 1,)), dma((octet - 1,)), dma((octet - 1,)),
        ],
        compiler_params=pltpu.CompilerParams(
            collective_id=0, has_side_effects=True, vmem_limit_bytes=48 << 20),
    )(coeffs, offs, pltpu.with_memory_space_constraint(probes, pltpu.HBM))
    scale = math.sqrt(rows * ns)
    tile = 1024
    q, u = pl.pallas_call(
        functools.partial(factor_kernel, scale),
        grid=(share // tile,),
        out_shape=(jax.ShapeDtypeStruct((share, k), F32), jax.ShapeDtypeStruct((k, k), F32)),
        in_specs=[hbm_spec, vmem_spec],
        out_specs=(pl.BlockSpec((tile, k), lambda i: (i, 0)), pl.BlockSpec((k, k), lambda i: (0, 0))),
        scratch_shapes=[pltpu.VMEM((2 * k, 2 * k), BF16), pltpu.VMEM((share, 2 * k), BF16), dma],
        compiler_params=pltpu.CompilerParams(dimension_semantics=("arbitrary",), vmem_limit_bytes=32 << 20),
    )(hl, gram)
    return q, u


def solution(mesh):
    in_specs = (P("space", None), P("rec", None, "space"), P("rec", None))
    out_specs = (P(("space", "rec"), None), P())
    body = functools.partial(local, mesh.shape["rec"], mesh.shape["space"])
    return jax.shard_map(body, mesh=mesh, in_specs=in_specs, out_specs=out_specs, check_vma=False)
```
